32 devices in a mesh: site: 8 (over z, y), ka: 4 (over x, core).
Axes of the slice: x: 2, y: 2, z: 4, core: 2. Of those that a mesh axis runs over, the one named last changes fastest.
Arguments:
- positions: float32 [3, 128], P(None, 'site'), may hold values from 0 to 1
- site_class: int32 [128], P('site'), may hold values from 0 to 3
- class_charge: float32 [4], replicated, may hold values from -2 to 2
- miller: int32 [3, 524288], P(None, 'ka'), may hold values from -80 to 80, as said below
Outputs:
- forces: float32 [3, 128], P(None, ('site', 'ka'))
- energy: float32 [], replicated
The draws below stay inside these ranges and needn't reach their ends.
Inputs may be any that keep to these rules, and one draw needn't show every extreme that they name: `miller`: the k-vectors are all distinct, and none has all three indices zero.
All inputs are finite; a program needn't handle non-finite values.
Results may differ from the reference program's by a relative error of at most 0.0003.
Values sent between devices are 32-bit elements; how exact they have to be, the bound alone decides.
A program may use at most 64 MiB of HBM per device.

```python
import math
import jax
import jax.numpy as jnp
from jax import lax

KBLOCK = 4096
MMAX = 80
NCLS = 4
NSITES = 128
KVECS = 524288


def draw_miller(key, part):
    side = 2 * MMAX + 1
    cube = side * side * side
    centre = (cube - 1) // 2
    order = jax.random.permutation(jax.random.fold_in(key, 11), cube - 1).astype(jnp.int32)
    picked = order[:KVECS]
    picked = jnp.where(picked >= centre, picked + 1, picked)
    first = picked // (side * side) - MMAX
    second = picked // side % side - MMAX
    third = picked % side - MMAX
    return jnp.stack([first, second, third], axis=0).astype(jnp.int32)


def place_ends(values, rng, low, top_value):
    longest = values.shape.index(max(values.shape))
    spots = []
    for shift in (0, 1):
        where = [jax.random.randint(jax.random.fold_in(rng, axis), (), 0, length) for axis, length in enumerate(values.shape)]
        where[longest] = (where[longest] + shift) % values.shape[longest]
        spots.append(tuple(where))
    return values.at[spots[0]].set(low).at[spots[1]].set(top_value)


def level_of(rng, extent, cuts, smallest, top_value):
    loudness, own = 1.0, jax.random.fold_in(rng, 6)
    for axis_at, shards_of in cuts:
        steps = jnp.exp(jax.random.uniform(jax.random.fold_in(own, axis_at), (shards_of,), jnp.float32, smallest / len(cuts), top_value / len(cuts)))
        loudness = loudness * jnp.repeat(steps, extent[axis_at] // shards_of).reshape([-1 if axis == axis_at else 1 for axis in range(len(extent))])
    return loudness


def setup_inputs(seed: int = 0) -> dict:
    key_of = jax.random.split(jax.random.key(seed), 5)
    positions = jnp.clip(1.0 * jax.random.uniform(key_of[0], (3, NSITES), jnp.float32) ** level_of(key_of[0], (3, NSITES), ((1, 8),), -0.2, 0.2), 0.0, 1.0)
    site_class = place_ends(jax.random.randint(key_of[1], (NSITES,), 0, NCLS), jax.random.fold_in(key_of[1], 1), 0, NCLS - 1).astype(jnp.int32)
    class_charge = jnp.clip(jax.random.uniform(key_of[2], (NCLS,), jnp.float32, -2.0, 2.0), -2.0, 2.0)
    miller = draw_miller(jax.random.fold_in(key_of[4], 71), 0)
    return dict(positions=positions, site_class=site_class, class_charge=class_charge, miller=miller)


def charges_of(site_class, class_charge):
    onehot = (site_class[None, :] == jnp.arange(NCLS, dtype=jnp.int32)[:, None]).astype(jnp.float32)
    return jnp.dot(class_charge, onehot, precision=lax.Precision.HIGHEST)

def kernel_weights(mfloat):
    square = lax.optimization_barrier(jnp.sum(mfloat * mfloat, axis=0))
    limit = float(MMAX * MMAX)
    return limit * jnp.exp(-square / limit) / square

def phases(mblock, positions):
    angles = 2.0 * math.pi * (mblock[0][:, None] * positions[0][None, :] + mblock[1][:, None] * positions[1][None, :] + mblock[2][:, None] * positions[2][None, :])
    return (jnp.cos(angles), jnp.sin(angles))

def reference(positions, site_class, class_charge, miller):
    charge = charges_of(site_class, class_charge)
    mfloat = miller.astype(jnp.float32)
    weights = kernel_weights(mfloat)
    blocks = KVECS // KBLOCK
    mblocks = mfloat.reshape(3, blocks, KBLOCK).transpose(1, 0, 2)
    scale = 1.0 / math.sqrt(NSITES)

    def factor(mblock):
        cosine, sine = phases(mblock, positions)
        return (jnp.dot(cosine, charge, precision=lax.Precision.HIGHEST) * scale, jnp.dot(sine, charge, precision=lax.Precision.HIGHEST) * scale)
    creal, cimag = lax.map(factor, mblocks)
    wblocks = weights.reshape(blocks, KBLOCK)
    energy = jnp.sum(wblocks * (creal * creal + cimag * cimag)) / KVECS

    def accumulate(total, items):
        mblock, real_part, imag_part, wblock = items
        cosine, sine = phases(mblock, positions)
        grad_sine = mblock * (wblock * real_part)[None, :]
        grad_cosine = mblock * (wblock * imag_part)[None, :]
        total = total + jnp.dot(grad_sine, sine, precision=lax.Precision.HIGHEST) - jnp.dot(grad_cosine, cosine, precision=lax.Precision.HIGHEST)
        return (total, None)
    total, unused = lax.scan(accumulate, jnp.zeros((3, NSITES), jnp.float32), (mblocks, creal, cimag, wblocks))
    forces = 4.0 * math.pi / math.sqrt(NSITES * KVECS) * charge[None, :] * total
    return (forces, energy)
```

```python
import functools
import math

import jax
import jax.numpy as jnp
from jax import lax
from jax.experimental import pallas as pl
from jax.experimental.pallas import tpu as pltpu
from jax.sharding import PartitionSpec as P

MMAX = 80
NCLS = 4
MESH = pl.DeviceIdType.MESH
F32 = jnp.float32
BF16 = jnp.bfloat16
A0, A1, A2 = 1.5707884689227576, -0.645711988911062, 0.07766738858001387
TINY = 1e-24
KB = 512
ROWS = 16


def kernel(
    nsite, nka, nsites, kvecs,
    pos_ref, cls_ref, cc_ref, mil_ref,
    out_ref, en_ref,
    mi, m16, wts, x16, alpha2, ca0, ca1, ca2, qabs, sh, ch, vbuf, facc, eacc, qtot,
    ag_out, ag_in, rs_out, rs_in,
    mil_sem, ag_send, ag_recv, rs_send, rs_recv,
):
    ndev = nsite * nka
    si, ki = lax.axis_index("site"), lax.axis_index("ka")
    me = si * nka + ki
    ls = pos_ref.shape[1]
    sub = mi.shape[1]
    spd = nsites // ndev
    nblk = sub // KB

    mil_copy = pltpu.make_async_copy(
        mil_ref.at[:, pl.ds(pl.multiple_of(si * sub, 128), sub)], mi, mil_sem
    )
    mil_copy.start()

    cls = cls_ref[...]
    charge = jnp.zeros(cls.shape, F32)
    for c in range(NCLS):
        charge = jnp.where(cls == c, cc_ref[c], charge)
    ag_out[...] = jnp.zeros_like(ag_out)
    ag_out[0:3, 0:ls] = pos_ref[...]
    ag_out[3:4, 0:ls] = charge

    barrier = pltpu.get_barrier_semaphore()

    @pl.loop(1, ndev)
    def _(i):
        to = lax.rem(me + i, ndev)
        pl.semaphore_signal(
            barrier, inc=1, device_id=(lax.div(to, nka), lax.rem(to, nka)), device_id_type=MESH
        )

    mil_copy.wait()

    @pl.loop(0, nblk)
    def _(b):
        at = pl.ds(pl.multiple_of(b * KB, KB), KB)
        m = mi[:, at].astype(F32)
        sq = jnp.sum(m * m, axis=0, keepdims=True)
        limit = float(MMAX * MMAX)
        wts[:, at] = limit * jnp.exp(sq * (-1.0 / limit)) / sq
        m16[:, at] = jnp.concatenate(
            [m, m, m, jnp.ones((1, KB), F32), jnp.zeros((6, KB), F32)], axis=0
        ).astype(BF16)

    pl.semaphore_wait(barrier, ndev - 1)

    def ag_copy(src, to):
        return pltpu.make_async_remote_copy(
            src_ref=ag_out, dst_ref=ag_in.at[src], send_sem=ag_send.at[to],
            recv_sem=ag_recv.at[src], device_id=(to, ki), device_id_type=MESH,
        )

    @pl.loop(1, nsite)
    def _(i):
        ag_copy(si, lax.rem(si + i, nsite)).start()

    ag_in[si] = ag_out[...]

    @pl.loop(1, nsite)
    def _(i):
        other = lax.rem(si + i, nsite)
        ag_copy(other, other).wait_recv()

    per = 128 // ls
    for t in range(nsites // 128):
        allrows = ag_in[t * per]
        for i in range(1, per):
            allrows = allrows + pltpu.roll(ag_in[t * per + i], i * ls, 1)
        x = allrows[0:3]
        x = x - jnp.round(x)
        q = allrows[3:4]
        x1 = x.astype(BF16).astype(F32)
        x2 = (x - x1).astype(BF16).astype(F32)
        x3 = x - x1 - x2
        half = jnp.where(q < 0.0, 0.5, 0.0)
        qc = jnp.maximum(jnp.abs(q), TINY)
        al2 = jnp.sqrt(qc)
        al = jnp.sqrt(al2)
        rows = jnp.concatenate(
            [x1, x2, x3, half, al2, al * A0, al * A1, al * A2, jnp.abs(q), qc,
             jnp.zeros((112, 128), F32)], axis=0
        )
        cols = rows.T
        rs_ = pl.ds(t * 128, 128)
        x16[rs_, :] = cols[:, 0:16].astype(BF16)
        alpha2[rs_, :] = jnp.broadcast_to(cols[:, 10:11], (128, 128))
        ca0[rs_, :] = jnp.broadcast_to(cols[:, 11:12], (128, 128))
        ca1[rs_, :] = jnp.broadcast_to(cols[:, 12:13], (128, 128))
        ca2[rs_, :] = jnp.broadcast_to(cols[:, 13:14], (128, 128))
        qabs[rs_, 0:2] = cols[:, 14:16]
        total = jnp.broadcast_to(jnp.sum(qc, axis=1, keepdims=True), (1, 128))
        qtot[...] = total if t == 0 else qtot[...] + total

    facc[...] = jnp.zeros_like(facc)
    eacc[...] = jnp.zeros_like(eacc)
    isn = 1.0 / math.sqrt(nsites)

    def wide(v):
        return jnp.concatenate([v] * (KB // 128), axis=1)

    @pl.loop(0, nblk)
    def _(b):
        at = pl.ds(pl.multiple_of(b * KB, KB), KB)
        mb = m16[:, at]
        turns = jnp.dot(x16[...], mb, preferred_element_type=F32)
        sums = sumc = None
        for j in range(nsites // ROWS):
            rr = slice(j * ROWS, (j + 1) * ROWS)
            t = turns[rr]
            r = t - jnp.round(t)
            z = r * r
            s = r * (wide(ca0[rr]) + z * (wide(ca1[rr]) + z * wide(ca2[rr])))
            s2 = s * s
            u = wide(alpha2[rr]) - s2
            sc = s * (u * lax.rsqrt(u))
            dc = u - s2
            sj = sc * dc
            cj = sc * sc
            sh[rr] = sj
            ch[rr] = cj
            sums = sj if j == 0 else sums + sj
            sumc = cj if j == 0 else sumc + cj
        cimag = (4.0 * isn) * jnp.sum(sums, axis=0, keepdims=True)
        creal = isn * (wide(qtot[...]) - 8.0 * jnp.sum(sumc, axis=0, keepdims=True))
        w = wts[:, at]
        g1 = w * creal
        g2 = w * cimag
        eacc[...] += g1 * creal + g2 * cimag
        g2 = 2.0 * g2

        def split(v, rows):
            hi = v.astype(BF16)
            vbuf[rows, 0:KB] = hi
            vbuf[rows, KB:] = (v - hi.astype(F32)).astype(BF16)

        for j in range(nsites // ROWS):
            rr = slice(j * ROWS, (j + 1) * ROWS)
            split(sh[rr] * g1 + ch[rr] * g2, rr)
        split(jnp.broadcast_to(g2, (ROWS, KB)), slice(nsites, nsites + ROWS))
        facc[...] += lax.dot_general(
            vbuf[...], jnp.concatenate([mb, mb], axis=1), (((1,), (1,)), ((), ())),
            preferred_element_type=F32,
        )

    energy = jnp.sum(eacc[...], axis=1, keepdims=True) * (1.0 / kvecs)
    fscale = 4.0 * math.pi / math.sqrt(nsites * kvecs)
    qa, qc = qabs[:, 0:1], qabs[:, 1:2]
    forces = (fscale * (qa / qc)) * (4.0 * facc[0:nsites] - (0.5 * qc) * facc[nsites : nsites + 1])
    lane = lax.broadcasted_iota(jnp.int32, forces.shape, 1)
    forces = jnp.where(lane == 3, energy, forces)
    rs_out[...] = jnp.zeros_like(rs_out)
    for p in range(ndev):
        rs_out[p, :, 0:16] = forces[p * spd : (p + 1) * spd]

    def rs_copy(src, to):
        return pltpu.make_async_remote_copy(
            src_ref=rs_out.at[to], dst_ref=rs_in.at[src], send_sem=rs_send.at[to],
            recv_sem=rs_recv.at[src], device_id=(lax.div(to, nka), lax.rem(to, nka)),
            device_id_type=MESH,
        )

    @pl.loop(1, ndev)
    def _(i):
        rs_copy(me, lax.rem(me + i, ndev)).start()

    rs_in[me] = rs_out[me]

    @pl.loop(1, ndev)
    def _(i):
        other = lax.rem(me + i, ndev)
        rs_copy(other, me).wait_recv()

    mine = jnp.sum(rs_in[...], axis=0)
    sub_i = lax.broadcasted_iota(jnp.int32, (spd, 128), 0)
    lane_i = lax.broadcasted_iota(jnp.int32, (spd, 128), 1)
    for d in range(3):
        row = jnp.sum(jnp.where(sub_i == lane_i, mine[:, d : d + 1], 0.0), axis=0, keepdims=True)
        out_ref[d : d + 1, :] = row[:, 0:spd]
    en_ref[...] = mine[0:1, 3:4]

    @pl.loop(1, ndev)
    def _(i):
        rs_copy(me, lax.rem(me + i, ndev)).wait_send()

    @pl.loop(1, nsite)
    def _(i):
        ag_copy(si, lax.rem(si + i, nsite)).wait_send()


def local(nsite, nka, positions, site_class, class_charge, miller):
    ndev = nsite * nka
    ls = positions.shape[1]
    nsites = ls * nsite
    kvecs = miller.shape[1] * nka
    sub = miller.shape[1] // nsite
    spd = nsites // ndev
    vmem = pl.BlockSpec(memory_space=pltpu.VMEM)
    forces, energy = pl.pallas_call(
        functools.partial(kernel, nsite, nka, nsites, kvecs),
        out_shape=(jax.ShapeDtypeStruct((3, spd), F32), jax.ShapeDtypeStruct((1, 1), F32)),
        in_specs=[
            vmem, vmem, pl.BlockSpec(memory_space=pltpu.SMEM), pl.BlockSpec(memory_space=pl.ANY),
        ],
        out_specs=(vmem, vmem),
        scratch_shapes=[
            pltpu.VMEM((3, sub), jnp.int32),
            pltpu.VMEM((16, sub), BF16),
            pltpu.VMEM((1, sub), F32),
            pltpu.VMEM((nsites, 16), BF16),
            pltpu.VMEM((nsites, 128), F32),
            pltpu.VMEM((nsites, 128), F32),
            pltpu.VMEM((nsites, 128), F32),
            pltpu.VMEM((nsites, 128), F32),
            pltpu.VMEM((nsites, 128), F32),
            pltpu.VMEM((nsites, KB), F32),
            pltpu.VMEM((nsites, KB), F32),
            pltpu.VMEM((nsites + ROWS, 2 * KB), BF16),
            pltpu.VMEM((nsites + ROWS, 16), F32),
            pltpu.VMEM((1, KB), F32),
            pltpu.VMEM((1, 128), F32),
            pltpu.VMEM((8, 128), F32),
            pltpu.VMEM((nsite, 8, 128), F32),
            pltpu.VMEM((ndev, spd, 128), F32),
            pltpu.VMEM((ndev, spd, 128), F32),
            pltpu.SemaphoreType.DMA,
            pltpu.SemaphoreType.DMA((nsite,)),
            pltpu.SemaphoreType.DMA((nsite,)),
            pltpu.SemaphoreType.DMA((ndev,)),
            pltpu.SemaphoreType.DMA((ndev,)),
        ],
        compiler_params=pltpu.CompilerParams(collective_id=0, has_side_effects=True),
        name="ewald",
    )(positions, site_class.reshape(1, ls), class_charge, miller)
    return forces, energy[0, 0]


def solution(mesh):
    placed = (P(None, "site"), P("site"), P(), P(None, "ka"))
    return jax.shard_map(
        functools.partial(local, mesh.shape["site"], mesh.shape["ka"]),
        mesh=mesh,
        in_specs=placed,
        out_specs=(P(None, ("site", "ka")), P()),
        check_vma=False,
    )
```

```python
import functools
import math

import jax
import jax.numpy as jnp
from jax import lax
from jax.experimental import pallas as pl
from jax.experimental.pallas import tpu as pltpu
from jax.sharding import PartitionSpec as P

MMAX = 80
NCLS = 4
MESH = pl.DeviceIdType.MESH
F32 = jnp.float32
BF16 = jnp.bfloat16
A0, A1, A2 = 1.5707884689227576, -0.645711988911062, 0.07766738858001387
TINY = 1e-24
KB = 512
ROWS = 16


def kernel(
    nsite, nka, nsites, kvecs,
    pos_ref, cls_ref, cc_ref, mil_ref,
    out_ref, en_ref,
    mi, m16, wts, x16, alpha2, ca0, ca1, ca2, qabs, sh, ch, vbuf, facc, eacc, qtot, tbuf, gr1, gr2,
    ag_out, ag_in, rs_out, rs_in,
    mil_sem, ag_send, ag_recv, rs_send, rs_recv,
):
    ndev = nsite * nka
    si, ki = lax.axis_index("site"), lax.axis_index("ka")
    me = si * nka + ki
    ls = pos_ref.shape[1]
    sub = mi.shape[1]
    spd = nsites // ndev
    nblk = sub // KB

    mil_copy = pltpu.make_async_copy(
        mil_ref.at[:, pl.ds(pl.multiple_of(si * sub, 128), sub)], mi, mil_sem
    )
    mil_copy.start()

    cls = cls_ref[...]
    charge = jnp.zeros(cls.shape, F32)
    for c in range(NCLS):
        charge = jnp.where(cls == c, cc_ref[c], charge)
    ag_out[...] = jnp.zeros_like(ag_out)
    ag_out[0:3, 0:ls] = pos_ref[...]
    ag_out[3:4, 0:ls] = charge

    barrier = pltpu.get_barrier_semaphore()

    @pl.loop(1, ndev)
    def _(i):
        to = lax.rem(me + i, ndev)
        pl.semaphore_signal(
            barrier, inc=1, device_id=(lax.div(to, nka), lax.rem(to, nka)), device_id_type=MESH
        )

    mil_copy.wait()

    @pl.loop(0, nblk)
    def _(b):
        at = pl.ds(pl.multiple_of(b * KB, KB), KB)
        m = mi[:, at].astype(F32)
        sq = jnp.sum(m * m, axis=0, keepdims=True)
        limit = float(MMAX * MMAX)
        wts[:, at] = limit * jnp.exp(sq * (-1.0 / limit)) / sq
        m16[:, at] = jnp.concatenate(
            [m, m, m, jnp.ones((1, KB), F32), jnp.zeros((6, KB), F32)], axis=0
        ).astype(BF16)

    pl.semaphore_wait(barrier, ndev - 1)

    def ag_copy(src, to):
        return pltpu.make_async_remote_copy(
            src_ref=ag_out, dst_ref=ag_in.at[src], send_sem=ag_send.at[to],
            recv_sem=ag_recv.at[src], device_id=(to, ki), device_id_type=MESH,
        )

    @pl.loop(1, nsite)
    def _(i):
        ag_copy(si, lax.rem(si + i, nsite)).start()

    ag_in[si] = ag_out[...]

    @pl.loop(1, nsite)
    def _(i):
        other = lax.rem(si + i, nsite)
        ag_copy(other, other).wait_recv()

    per = 128 // ls
    for t in range(nsites // 128):
        allrows = ag_in[t * per]
        for i in range(1, per):
            allrows = allrows + pltpu.roll(ag_in[t * per + i], i * ls, 1)
        x = allrows[0:3]
        x = x - jnp.round(x)
        q = allrows[3:4]
        x1 = x.astype(BF16).astype(F32)
        x2 = (x - x1).astype(BF16).astype(F32)
        x3 = x - x1 - x2
        half = jnp.where(q < 0.0, 0.5, 0.0)
        qc = jnp.maximum(jnp.abs(q), TINY)
        al2 = jnp.sqrt(qc)
        al = jnp.sqrt(al2)
        rows = jnp.concatenate(
            [x1, x2, x3, half, al2, al * A0, al * A1, al * A2, jnp.abs(q), qc,
             jnp.zeros((112, 128), F32)], axis=0
        )
        cols = rows.T
        rs_ = pl.ds(t * 128, 128)
        x16[rs_, :] = cols[:, 0:16].astype(BF16)
        alpha2[rs_, :] = jnp.broadcast_to(cols[:, 10:11], (128, 128))
        ca0[rs_, :] = jnp.broadcast_to(cols[:, 11:12], (128, 128))
        ca1[rs_, :] = jnp.broadcast_to(cols[:, 12:13], (128, 128))
        ca2[rs_, :] = jnp.broadcast_to(cols[:, 13:14], (128, 128))
        qabs[rs_, 0:2] = cols[:, 14:16]
        total = jnp.broadcast_to(jnp.sum(qc, axis=1, keepdims=True), (1, 128))
        qtot[...] = total if t == 0 else qtot[...] + total

    facc[...] = jnp.zeros_like(facc)
    eacc[...] = jnp.zeros_like(eacc)
    isn = 1.0 / math.sqrt(nsites)

    def wide(v):
        return jnp.concatenate([v] * (KB // 128), axis=1)

    def cols_of(b):
        return pl.ds(pl.multiple_of(b * KB, KB), KB)

    def split(v, rows):
        hi = v.astype(BF16)
        vbuf[rows, 0:KB] = hi
        vbuf[rows, KB:] = (v - hi.astype(F32)).astype(BF16)

    def gather_forces(b):
        mb = m16[:, cols_of(b)]
        facc[...] += lax.dot_general(
            vbuf[...], jnp.concatenate([mb, mb], axis=1), (((1,), (1,)), ((), ())),
            preferred_element_type=F32,
        )

    def second(rr):
        split(sh[rr] * gr1[...] + ch[rr] * gr2[...], rr)

    extra = slice(nsites, nsites + ROWS)
    chunks = [slice(j * ROWS, (j + 1) * ROWS) for j in range(nsites // ROWS)]
    for buf in (sh, ch, gr1, gr2, vbuf):
        buf[...] = jnp.zeros_like(buf)
    tbuf[...] = jnp.dot(x16[...], m16[:, 0:KB], preferred_element_type=F32)

    @pl.loop(0, nblk)
    def _(b):
        gather_forces(jnp.maximum(b - 2, 0))
        turns = jnp.dot(
            x16[...], m16[:, cols_of(jnp.minimum(b + 1, nblk - 1))], preferred_element_type=F32
        )
        sums = sumc = None
        for j, rr in enumerate(chunks):
            second(rr)
            t = tbuf[rr]
            r = t - jnp.round(t)
            z = r * r
            s = r * (wide(ca0[rr]) + z * (wide(ca1[rr]) + z * wide(ca2[rr])))
            s2 = s * s
            u = wide(alpha2[rr]) - s2
            sc = s * (u * lax.rsqrt(u))
            dc = u - s2
            sj = sc * dc
            cj = sc * sc
            sh[rr] = sj
            ch[rr] = cj
            tbuf[rr] = turns[rr]
            sums = sj if j == 0 else sums + sj
            sumc = cj if j == 0 else sumc + cj
        split(jnp.broadcast_to(gr2[...], (ROWS, KB)), extra)
        cimag = (4.0 * isn) * jnp.sum(sums, axis=0, keepdims=True)
        creal = isn * (wide(qtot[...]) - 8.0 * jnp.sum(sumc, axis=0, keepdims=True))
        w = wts[:, cols_of(b)]
        g1 = w * creal
        g2 = w * cimag
        eacc[...] += g1 * creal + g2 * cimag
        gr1[...] = g1
        gr2[...] = 2.0 * g2

    gather_forces(max(nblk - 2, 0))
    for rr in chunks:
        second(rr)
    split(jnp.broadcast_to(gr2[...], (ROWS, KB)), extra)
    gather_forces(nblk - 1)

    energy = jnp.sum(eacc[...], axis=1, keepdims=True) * (1.0 / kvecs)
    fscale = 4.0 * math.pi / math.sqrt(nsites * kvecs)
    qa, qc = qabs[:, 0:1], qabs[:, 1:2]
    forces = (fscale * (qa / qc)) * (4.0 * facc[0:nsites] - (0.5 * qc) * facc[nsites : nsites + 1])
    lane = lax.broadcasted_iota(jnp.int32, forces.shape, 1)
    forces = jnp.where(lane == 3, energy, forces)
    rs_out[...] = jnp.zeros_like(rs_out)
    for p in range(ndev):
        rs_out[p, :, 0:16] = forces[p * spd : (p + 1) * spd]

    def rs_copy(src, to):
        return pltpu.make_async_remote_copy(
            src_ref=rs_out.at[to], dst_ref=rs_in.at[src], send_sem=rs_send.at[to],
            recv_sem=rs_recv.at[src], device_id=(lax.div(to, nka), lax.rem(to, nka)),
            device_id_type=MESH,
        )

    @pl.loop(1, ndev)
    def _(i):
        rs_copy(me, lax.rem(me + i, ndev)).start()

    rs_in[me] = rs_out[me]

    @pl.loop(1, ndev)
    def _(i):
        other = lax.rem(me + i, ndev)
        rs_copy(other, me).wait_recv()

    mine = jnp.sum(rs_in[...], axis=0)
    sub_i = lax.broadcasted_iota(jnp.int32, (spd, 128), 0)
    lane_i = lax.broadcasted_iota(jnp.int32, (spd, 128), 1)
    for d in range(3):
        row = jnp.sum(jnp.where(sub_i == lane_i, mine[:, d : d + 1], 0.0), axis=0, keepdims=True)
        out_ref[d : d + 1, :] = row[:, 0:spd]
    en_ref[...] = mine[0:1, 3:4]

    @pl.loop(1, ndev)
    def _(i):
        rs_copy(me, lax.rem(me + i, ndev)).wait_send()

    @pl.loop(1, nsite)
    def _(i):
        ag_copy(si, lax.rem(si + i, nsite)).wait_send()


def local(nsite, nka, positions, site_class, class_charge, miller):
    ndev = nsite * nka
    ls = positions.shape[1]
    nsites = ls * nsite
    kvecs = miller.shape[1] * nka
    sub = miller.shape[1] // nsite
    spd = nsites // ndev
    vmem = pl.BlockSpec(memory_space=pltpu.VMEM)
    forces, energy = pl.pallas_call(
        functools.partial(kernel, nsite, nka, nsites, kvecs),
        out_shape=(jax.ShapeDtypeStruct((3, spd), F32), jax.ShapeDtypeStruct((1, 1), F32)),
        in_specs=[
            vmem, vmem, pl.BlockSpec(memory_space=pltpu.SMEM), pl.BlockSpec(memory_space=pl.ANY),
        ],
        out_specs=(vmem, vmem),
        scratch_shapes=[
            pltpu.VMEM((3, sub), jnp.int32),
            pltpu.VMEM((16, sub), BF16),
            pltpu.VMEM((1, sub), F32),
            pltpu.VMEM((nsites, 16), BF16),
            pltpu.VMEM((nsites, 128), F32),
            pltpu.VMEM((nsites, 128), F32),
            pltpu.VMEM((nsites, 128), F32),
            pltpu.VMEM((nsites, 128), F32),
            pltpu.VMEM((nsites, 128), F32),
            pltpu.VMEM((nsites, KB), F32),
            pltpu.VMEM((nsites, KB), F32),
            pltpu.VMEM((nsites + ROWS, 2 * KB), BF16),
            pltpu.VMEM((nsites + ROWS, 16), F32),
            pltpu.VMEM((1, KB), F32),
            pltpu.VMEM((1, 128), F32),
            pltpu.VMEM((nsites, KB), F32),
            pltpu.VMEM((1, KB), F32),
            pltpu.VMEM((1, KB), F32),
            pltpu.VMEM((8, 128), F32),
            pltpu.VMEM((nsite, 8, 128), F32),
            pltpu.VMEM((ndev, spd, 128), F32),
            pltpu.VMEM((ndev, spd, 128), F32),
            pltpu.SemaphoreType.DMA,
            pltpu.SemaphoreType.DMA((nsite,)),
            pltpu.SemaphoreType.DMA((nsite,)),
            pltpu.SemaphoreType.DMA((ndev,)),
            pltpu.SemaphoreType.DMA((ndev,)),
        ],
        compiler_params=pltpu.CompilerParams(collective_id=0, has_side_effects=True),
        name="ewald",
    )(positions, site_class.reshape(1, ls), class_charge, miller)
    return forces, energy[0, 0]


def solution(mesh):
    placed = (P(None, "site"), P("site"), P(), P(None, "ka"))
    return jax.shard_map(
        functools.partial(local, mesh.shape["site"], mesh.shape["ka"]),
        mesh=mesh,
        in_specs=placed,
        out_specs=(P(None, ("site", "ka")), P()),
        check_vma=False,
    )
```
